32 devices in a mesh: ex: 4 (over y, x), ft: 8 (over z, core).
Axes of the slice: x: 2, y: 2, z: 4, core: 2. Of those that a mesh axis runs over, the one named last changes fastest.
Arguments:
- features: bfloat16 [512, 262144], P(('ex', 'ft')), may hold values from -0.0234375 to 0.0234375
- labels: int32 [512], P(('ex', 'ft')), may hold values 0 or 1
- start_weights: float32 [262144], P(('ex', 'ft')), may hold values from -6 to 6
- hist_s: float32 [20, 262144], P(None, ('ex', 'ft')), may hold values from -12 to 12
- hist_y: float32 [20, 262144], P(None, ('ex', 'ft')), may hold values from -30 to 30, as said below
Outputs:
- new_weights: float32 [262144], P(('ex', 'ft'))
- direction: float32 [262144], P(('ex', 'ft'))
The draws below stay inside these ranges and needn't reach their ends.
Inputs may be any that keep to these rules, and one draw needn't show every extreme that they name: Entry by entry, hist_y times hist_s is nonnegative, and every pair has a positive inner product; every entry of hist_y is at most 1.2 times the matching entry of hist_s in magnitude.
All inputs are finite; a program needn't handle non-finite values. No bound on the sum of `labels` on one device may be relied on, other than what follows from the above.
Results may differ from the reference program's by a relative error of at most 0.0081.
Values may be sent and summed in bfloat16 or wider, within the bound.
A program may use at most 64 MiB of HBM per device.

```python
import jax
import jax.numpy as jnp
from jax import lax

F = 262144
HIST = 20
ITERS = 2
EXAMPLES = 512


def history_pair(key):
    base = jax.random.fold_in(key, 11)
    key_s, key_c, key_u, key_b = jax.random.split(base, 4)
    block_scale = jnp.exp(jax.random.uniform(key_b, (HIST, F // 128), jnp.float32, jnp.log(0.3), jnp.log(3.0)))
    block_scale = jnp.repeat(block_scale, 128, axis=1)
    plain = jnp.clip(jax.random.normal(key_s, (HIST, F), jnp.float32), -4.0, 4.0)
    curve = jnp.exp(jax.random.uniform(key_c, (HIST, F), jnp.float32, jnp.log(0.35), jnp.log(1.0)))
    steps = plain * block_scale
    noise = jax.random.uniform(key_u, (HIST, F), jnp.float32, -1.0, 1.0)
    diffs = curve * steps + 0.2 * curve * noise * jnp.abs(steps)
    return (steps, diffs)


def draw_hist_s(key, part):
    return history_pair(key)[0]


def draw_hist_y(key, part):
    return history_pair(key)[1]


def place_ends(result, rng, least, largest):
    longest = result.shape.index(max(result.shape))
    spots = []
    for shift in (0, 1):
        where = [jax.random.randint(jax.random.fold_in(rng, axis), (), 0, length) for axis, length in enumerate(result.shape)]
        where[longest] = (where[longest] + shift) % result.shape[longest]
        spots.append(tuple(where))
    return result.at[spots[0]].set(least).at[spots[1]].set(largest)


def raised(result, own_key, source, target, parts, factor):
    owner, partner = [(jnp.arange(result.shape[axis_at]) // (result.shape[axis_at] // parts)).reshape([-1 if axis == axis_at else 1 for axis in range(result.ndim)]) for axis_at in (source, target)]
    chosen = jax.random.permutation(own_key, parts)[partner]
    strong = (owner == chosen) | (owner == (partner + parts // 2) % parts)
    return jnp.where(strong, factor * result, result)


def levels(key, extent, shards, low, high):
    def one(dim, blocks):
        draws = jax.random.uniform(jax.random.fold_in(jax.random.fold_in(key, 6), dim), (blocks,), jnp.float32, low / len(shards), high / len(shards))
        return jnp.repeat(jnp.exp(draws), extent[dim] // blocks).reshape((-1,) + (1,) * (len(extent) - dim - 1))

    level = one(*shards[0])
    for cut in shards[1:]:
        level = level * one(*cut)
    return level


def normal_values(rng, dims, scale, reach, shards=(), kind=jnp.bfloat16):
    result = scale * jax.random.normal(rng, dims, jnp.float32)
    if shards:
        result = result * levels(rng, dims, shards, -0.22, 0.18)
    return jnp.clip(result, -reach, reach).astype(kind)


def gaussian_with(stream_key, dims, deviation, reach, cuts, heavy, dtype=jnp.bfloat16):
    result = deviation * jax.random.normal(stream_key, dims, jnp.float32)
    if cuts:
        result = result * levels(stream_key, dims, cuts, -0.22, 0.18)
    return jnp.clip(raised(result, jax.random.fold_in(stream_key, 3), *heavy), -reach, reach).astype(dtype)


def setup_inputs(seed: int = 0) -> dict:
    arg_keys = jax.random.split(jax.random.key(seed), 6)
    return {
        "features": gaussian_with(arg_keys[0], (EXAMPLES, F), F ** -0.5, 0.0234375, ((0, 32),), (0, 1, 32, 2.75)),
        "labels": place_ends((jax.random.randint(arg_keys[1], (EXAMPLES,), 0, 2) < 1).astype(jnp.int32), jax.random.fold_in(arg_keys[1], 1), 0, 1),
        "start_weights": normal_values(arg_keys[2], (F,), 1.0, 6.0, ((0, 32),), jnp.float32),
        "hist_s": draw_hist_s(jax.random.fold_in(arg_keys[5], 71), 0),
        "hist_y": draw_hist_y(jax.random.fold_in(arg_keys[5], 71), 0),
    }


def two_loop(gram):
    pairs = (gram.shape[0] - 1) // 2
    delta = jnp.zeros((gram.shape[0],), jnp.float32).at[2 * pairs].set(-1.0)
    alphas = [None] * pairs
    for index in reversed(range(pairs)):
        alpha = jnp.sum(delta * gram[:, index]) / gram[index, pairs + index]
        delta = delta.at[pairs + index].add(-alpha)
        alphas[index] = alpha
    delta = delta * (gram[pairs - 1, 2 * pairs - 1] / gram[2 * pairs - 1, 2 * pairs - 1])
    for index in range(pairs):
        beta = jnp.sum(delta * gram[pairs + index, :]) / gram[index, pairs + index]
        delta = delta.at[index].add(alphas[index] - beta)
    return delta


def reference(features, labels, start_weights, hist_s, hist_y):
    weights = start_weights
    stored_s, stored_y = hist_s, hist_y
    prev_weights = weights
    prev_grad = weights
    direction = weights
    for step in range(ITERS):
        margin = jnp.dot(features, weights.astype(jnp.bfloat16), preferred_element_type=jnp.float32)
        resid = (jax.nn.sigmoid(margin) - labels.astype(jnp.float32)).astype(jnp.bfloat16)
        grad = jnp.dot(resid, features, preferred_element_type=jnp.float32) + 0.1 * weights
        if step > 0:
            stored_s = jnp.concatenate([stored_s[1:], (weights - prev_weights)[None]], axis=0)
            stored_y = jnp.concatenate([stored_y[1:], (grad - prev_grad)[None]], axis=0)
        basis = jnp.concatenate([stored_s, stored_y, grad[None]], axis=0)
        gram = jnp.dot(basis, basis.T, precision=lax.Precision.HIGHEST, preferred_element_type=jnp.float32)
        delta = two_loop(gram)
        direction = jnp.dot(delta, basis, precision=lax.Precision.HIGHEST, preferred_element_type=jnp.float32)
        prev_weights, prev_grad = weights, grad
        weights = weights + direction
    return weights, direction
```

```python
import functools

import jax
import jax.numpy as jnp
from jax import lax
from jax.experimental import pallas as pl
from jax.experimental.pallas import tpu as pltpu
from jax.sharding import PartitionSpec as P

ITERS = 2
LANES = 128
MESH = pl.DeviceIdType.MESH
HIGH = lax.Precision.HIGHEST


def kernel(ne, nf, features, labels, weights, hist_s, hist_y, new_weights, direction,
           feat, s, y, wbf, wf, wg, sib_out, sib_in, own, chip_out, chip_in,
           grads, rows_out, rows_in, bf_out, bf_in, ac, bc, atc,
           feat_sem, hist_sem, ag_send, ag_recv, fw_send, fw_recv,
           sb_send, sb_recv, cp_send, cp_recv, ar_send, ar_recv, bf_send, bf_recv):
    nd = ne * nf
    chips = nd // 2
    examples = features.shape[0]
    rows = weights.shape[0]
    pairs = hist_s.shape[0]
    f32, bf16 = jnp.float32, jnp.bfloat16
    me = lax.axis_index("ex") * nf + lax.axis_index("ft")
    chip, core = me // 2, me % 2
    sibling = 2 * chip + (1 - core)

    def at(device):
        return (device // nf, device % nf)

    def remote(src, dst, send, recv, device):
        return pltpu.make_async_remote_copy(
            src_ref=src, dst_ref=dst, send_sem=send, recv_sem=recv,
            device_id=at(device), device_id_type=MESH)

    parts = feat_sem.shape[0]
    width = features.shape[1] // parts
    loads = [pltpu.make_async_copy(features.at[:, pl.ds(i * width, width)],
                                   feat.at[:, pl.ds(i * width, width)], feat_sem.at[i])
             for i in range(parts)]
    hist_loads = [pltpu.make_async_copy(hist_s, s, hist_sem.at[0]),
                  pltpu.make_async_copy(hist_y, y, hist_sem.at[1])]
    barrier = pltpu.get_barrier_semaphore()

    def greet(k, carry):
        pl.semaphore_signal(barrier, inc=1, device_id=at((me + k) % nd), device_id_type=MESH)
        return carry

    lax.fori_loop(1, nd, greet, 0)
    for copy in hist_loads + loads:
        copy.start()
    wbf[0] = weights[...].astype(bf16)
    wf[0] = weights[...]
    wg[0, me] = weights[...].astype(bf16)
    pl.semaphore_wait(barrier, nd - 1)

    def ag_copy(it, k):
        return remote(wbf.at[it], wg.at[it, me], ag_send.at[it, k], ag_recv.at[it, k],
                      2 * ((chip + k) % chips) + core)

    def fw_copy(it, k):
        block = 2 * ((chip - k + chips) % chips) + core
        return remote(wbf.at[it] if isinstance(k, int) else wg.at[it, block],
                      wg.at[it, block], fw_send.at[it, k], fw_recv.at[it, k], sibling)

    def gather_start(it):
        fw_copy(it, 0).start()

        def go(k, carry):
            ag_copy(it, k).start()
            return carry

        lax.fori_loop(1, chips, go, 0)

    def dot_block(it, device, acc):
        for half in range(rows // 16):
            w16 = wg[it, device, pl.ds(half * 16, 16), :].astype(f32)
            start = pl.multiple_of((device * rows + half * 16) * LANES, 16 * LANES)
            tile = feat[:, pl.ds(start, 16 * LANES)]
            for r in range(16):
                acc = acc + tile[:, r * LANES:(r + 1) * LANES].astype(f32) * w16[r:r + 1, :]
        return acc

    bits = bf_out.shape[0] - 1

    def bf_copy(b):
        step = 2 ** b
        partner = me + step * (1 - 2 * ((me // step) % 2))
        return remote(bf_out.at[b], bf_in.at[b], bf_send.at[b], bf_recv.at[b], partner)

    progress = [0]

    def advance():
        b = progress[0]
        if b < bits:
            bf_copy(b).wait()
            bf_out[b + 1] = bf_out[b] + bf_in[b]
            if b + 1 < bits:
                bf_copy(b + 1).start()
            progress[0] = b + 1

    sub = lax.broadcasted_iota(jnp.int32, (pairs, LANES), 0)
    lane = lax.broadcasted_iota(jnp.int32, (pairs, LANES), 1)

    def to_row(acc, offset):
        col = jnp.sum(acc, axis=1, keepdims=True)
        return jnp.sum(jnp.where(lane == sub + offset, col, 0.0), axis=0, keepdims=True)

    def to_col(row, offset):
        col = jnp.sum(jnp.where(lane == sub + offset, row, 0.0), axis=1, keepdims=True)
        return jnp.broadcast_to(col, (pairs, LANES))

    def all_sub(col):
        return jnp.broadcast_to(jnp.sum(col, axis=0, keepdims=True), (pairs, LANES))

    def spread(col, k):
        return jnp.broadcast_to(col[k:k + 1, :], (pairs, LANES))

    def ar_copy(it, k):
        return remote(rows_out.at[it], rows_in.at[it, k], ar_send.at[it, k], ar_recv.at[it, k],
                      (me + k) % nd)

    gather_start(0)
    hist_loads[0].wait()
    hist_loads[1].wait()

    chunk = min(1024, rows * LANES)
    contract = (((1,), (1,)), ((), ()))

    def products(i, sums):
        a = s[:, pl.ds(pl.multiple_of(i * chunk, chunk), chunk)]
        b = y[:, pl.ds(pl.multiple_of(i * chunk, chunk), chunk)]
        dot = functools.partial(lax.dot_general, dimension_numbers=contract, precision=HIGH,
                                preferred_element_type=f32)
        return (sums[0] + dot(a, b), sums[1] + dot(b, a), sums[2] + dot(b, b))

    zero = jnp.zeros((pairs, pairs), f32)
    sy, ys, yy = lax.fori_loop(0, rows * LANES // chunk, products, (zero, zero, zero))
    pad = jnp.zeros((pairs, LANES - 3 * pairs), f32)
    bf_out[0] = jnp.concatenate([sy, ys, yy, pad], axis=1)
    bf_copy(0).start()
    for copy in loads:
        copy.wait()

    for it in range(ITERS):
        acc = dot_block(it, me, jnp.zeros((examples, LANES), f32))

        def direct(k, acc):
            ag_copy(it, k).wait_recv()
            fw_copy(it, k).start()
            return dot_block(it, 2 * ((chip - k + chips) % chips) + core, acc)

        acc = lax.fori_loop(1, chips, direct, acc)
        advance()

        def forwarded(k, acc):
            fw_copy(it, k).wait_recv()
            return dot_block(it, 2 * ((chip - k + chips) % chips) + 1 - core, acc)

        fw_copy(it, 0).wait_recv()
        acc = dot_block(it, sibling, acc)
        acc = lax.fori_loop(1, chips, forwarded, acc)
        advance()
        margin = jnp.sum(acc, axis=1, keepdims=True)
        wide = 16 * examples
        on_diag = (lax.broadcasted_iota(jnp.int32, (examples, examples), 0)
                   == lax.broadcasted_iota(jnp.int32, (examples, examples), 1))
        label = jnp.sum(jnp.where(on_diag, labels[...].astype(f32), 0.0), axis=1, keepdims=True)
        resid = (1.0 / (1.0 + jnp.exp(-margin)) - label).astype(bf16).astype(f32)
        esub = lax.broadcasted_iota(jnp.int32, (examples, wide), 0)
        elane = lax.broadcasted_iota(jnp.int32, (examples, wide), 1)
        flat = jnp.sum(jnp.where(elane % examples == esub, resid, 0.0), axis=0, keepdims=True)
        gsub = lax.broadcasted_iota(jnp.int32, (16, wide), 0)
        glane = lax.broadcasted_iota(jnp.int32, (16, wide), 1)
        select = jnp.where(glane // examples == gsub, flat, 0.0).astype(bf16)

        def terms(device, part):
            start = pl.multiple_of((device * rows + part * 16) * LANES, 16 * LANES)
            tile = feat[:, pl.ds(start, 16 * LANES)]
            stack = jnp.concatenate(
                [tile[:, r * LANES:(r + 1) * LANES] for r in range(16)], axis=0)
            return jnp.dot(select, stack, preferred_element_type=f32)

        def sb_copy(k):
            return remote(sib_out.at[it, k], sib_in.at[it, k], sb_send.at[it, k],
                          sb_recv.at[it, k], sibling)

        def cp_copy(k):
            return remote(chip_out.at[it, k], chip_in.at[it, k], cp_send.at[it, k],
                          cp_recv.at[it, k], 2 * ((chip + k) % chips) + core)

        def compute(k):
            target = 2 * ((chip + k) % chips)
            for part in range(rows // 16):
                sib_out[it, k, pl.ds(part * 16, 16), :] = terms(target + 1 - core, part).astype(bf16)
            sb_copy(k).start()
            for part in range(rows // 16):
                own[k, pl.ds(part * 16, 16), :] = terms(target + core, part)

        def relay(k):
            sb_copy(k).wait_recv()
            chip_out[it, k] = (own[k] + sib_in[it, k].astype(f32)).astype(bf16)
            cp_copy(k).start()

        lag = min(3, chips - 1)

        def ahead(k, carry):
            compute(k)
            return carry

        def both(k, carry):
            compute(k)
            relay(k - lag)
            return carry

        def behind(k, carry):
            relay(k)
            return carry

        lax.fori_loop(1, 1 + lag, ahead, 0)
        lax.fori_loop(1 + lag, chips, both, 0)
        compute(0)
        lax.fori_loop(chips - lag, chips, behind, 0)
        advance()
        sb_copy(0).wait_recv()
        total = own[0] + sib_in[it, 0].astype(f32)

        def collect(k, total):
            cp_copy(k).wait_recv()
            return total + chip_in[it, k].astype(f32)

        total = lax.fori_loop(1, chips, collect, total)
        advance()
        w = wf[it]
        grad = total + 0.1 * w
        grads[it] = grad

        if it > 0:
            grads[ITERS + it] = grad - grads[it - 1]
            wf[ITERS + it] = w - wf[it - 1]
            for r in range(rows):
                s[0:1, r * LANES:(r + 1) * LANES] = wf[ITERS + it, r:r + 1, :]
                y[0:1, r * LANES:(r + 1) * LANES] = grads[ITERS + it, r:r + 1, :]
        accs = [jnp.zeros((pairs, LANES), f32) for _ in range(4 if it > 0 else 2)]
        for r in range(rows):
            st = s[:, r * LANES:(r + 1) * LANES]
            yt = y[:, r * LANES:(r + 1) * LANES]
            g = grads[it, r:r + 1, :]
            accs[0] = accs[0] + st * g
            accs[1] = accs[1] + yt * g
            if it > 0:
                dg = grads[ITERS + it, r:r + 1, :]
                accs[2] = accs[2] + st * dg
                accs[3] = accs[3] + yt * dg
        packed = to_row(accs[0], 0)
        for i in range(1, len(accs)):
            packed = packed + to_row(accs[i], i * pairs)
        rows_out[it] = packed
        rows_in[it, 0] = packed

        def ar_start(k, carry):
            ar_copy(it, k).start()
            return carry

        def ar_wait(k, carry):
            ar_copy(it, k).wait_recv()
            return carry

        lax.fori_loop(1, nd, ar_start, 0)
        if it == 0:
            while progress[0] < bits:
                advance()
            gram = bf_out[bits]
            diag = to_col(gram, 0)
            dinv = 1.0 / diag
            for k in range(pairs):
                col = jnp.broadcast_to(gram[:, k:k + 1], (pairs, LANES))
                ac[k] = jnp.where(sub < k, col * dinv, 0.0)
                col = jnp.broadcast_to(gram[:, pairs + k:pairs + k + 1], (pairs, LANES))
                atc[k] = jnp.where(sub > k, col * dinv, 0.0)
                bc[k] = jnp.broadcast_to(gram[:, 2 * pairs + k:2 * pairs + k + 1], (pairs, LANES))
            last = pairs - 1
            gamma = spread(diag, last) / spread(bc[last], last)
        lax.fori_loop(1, nd, ar_wait, 0)
        summed = jnp.sum(rows_in[it], axis=0)
        p, q = to_col(summed, 0), to_col(summed, pairs)

        first = sub == 0
        if it > 0:
            sdy, ydy = to_col(summed, 2 * pairs), to_col(summed, 3 * pairs)
            diag = jnp.where(first, sdy, diag)
            dinv = 1.0 / diag
            gamma = spread(sdy, 0) / spread(ydy, 0)
        t, v = -p * dinv, q
        if it > 0:
            a = spread(t, 0)
            t = t - a * jnp.where(first, 0.0, sdy * dinv)
            v = v + a * ydy
        for k in reversed(range(min(it, 1), pairs)):
            a = spread(t, k)
            column = ac[k]
            if it > 0:
                column = jnp.where(first, 0.0, column)
            t = t - a * column
            v = v + a * bc[k]
        if it > 0:
            v = jnp.where(first, q + all_sub(t * ydy), v)
        u = t + gamma * v * dinv
        for k in range(min(it, 1), pairs):
            u = u - spread(u, k) * atc[k]
        if it > 0:
            u = jnp.where(first, u - all_sub(jnp.where(first, 0.0, u * sdy)) * dinv, u)
        cy = -gamma * t
        cg = gamma[0:1, :]
        for r in range(rows):
            st = s[:, r * LANES:(r + 1) * LANES]
            yt = y[:, r * LANES:(r + 1) * LANES]
            step = jnp.sum(st * u + yt * cy, axis=0, keepdims=True) - cg * grads[it, r:r + 1, :]
            direction[r:r + 1, :] = step
        w = w + direction[...]
        if it + 1 < ITERS:
            wf[it + 1] = w
            wbf[it + 1] = w.astype(bf16)
            wg[it + 1, me] = w.astype(bf16)
            gather_start(it + 1)
        else:
            new_weights[...] = w

        def drain_chips(k, carry):
            ag_copy(it, k).wait_send()
            fw_copy(it, k).wait_send()
            sb_copy(k).wait_send()
            cp_copy(k).wait_send()
            return carry

        def drain_all(k, carry):
            ar_copy(it, k).wait_send()
            return carry

        fw_copy(it, 0).wait_send()
        sb_copy(0).wait_send()
        lax.fori_loop(1, chips, drain_chips, 0)
        lax.fori_loop(1, nd, drain_all, 0)


def per_device(ne, nf, features, labels, start_weights, hist_s, hist_y):
    nd = ne * nf
    chips = nd // 2
    bits = nd.bit_length() - 1
    examples = features.shape[0]
    size = start_weights.shape[0]
    pairs = hist_s.shape[0]
    rows = size // LANES
    f32, bf16 = jnp.float32, jnp.bfloat16
    vmem, dma = pltpu.VMEM, pltpu.SemaphoreType.DMA
    block = jax.ShapeDtypeStruct((rows, LANES), f32)
    in_vmem = pl.BlockSpec(memory_space=pltpu.VMEM)
    in_hbm = pl.BlockSpec(memory_space=pl.ANY)
    out = pl.pallas_call(
        functools.partial(kernel, ne, nf),
        out_shape=(block, block),
        in_specs=[in_hbm, in_vmem, in_vmem, in_hbm, in_hbm],
        out_specs=(in_vmem, in_vmem),
        scratch_shapes=[
            vmem(features.shape, bf16),
            vmem(hist_s.shape, f32),
            vmem(hist_y.shape, f32),
            vmem((ITERS, rows, LANES), bf16),
            vmem((2 * ITERS, rows, LANES), f32),
            vmem((ITERS, nd, rows, LANES), bf16),
            vmem((ITERS, chips, rows, LANES), bf16),
            vmem((ITERS, chips, rows, LANES), bf16),
            vmem((chips, rows, LANES), f32),
            vmem((ITERS, chips, rows, LANES), bf16),
            vmem((ITERS, chips, rows, LANES), bf16),
            vmem((2 * ITERS, rows, LANES), f32),
            vmem((ITERS, 1, LANES), f32),
            vmem((ITERS, nd, 1, LANES), f32),
            vmem((bits + 1, pairs, LANES), f32),
            vmem((bits, pairs, LANES), f32),
            vmem((pairs, pairs, LANES), f32),
            vmem((pairs, pairs, LANES), f32),
            vmem((pairs, pairs, LANES), f32),
            dma((8,)), dma((2,)),
            dma((ITERS, chips)), dma((ITERS, chips)),
            dma((ITERS, chips)), dma((ITERS, chips)),
            dma((ITERS, chips)), dma((ITERS, chips)),
            dma((ITERS, chips)), dma((ITERS, chips)),
            dma((ITERS, nd)), dma((ITERS, nd)),
            dma((bits,)), dma((bits,)),
        ],
        compiler_params=pltpu.CompilerParams(collective_id=0, has_side_effects=True),
    )(features, labels.reshape(1, examples), start_weights.reshape(rows, LANES), hist_s, hist_y)
    return out[0].reshape(size), out[1].reshape(size)


def solution(mesh):
    return jax.shard_map(
        functools.partial(per_device, mesh.shape["ex"], mesh.shape["ft"]),
        mesh=mesh,
        in_specs=(
            P(("ex", "ft"), None),
            P(("ex", "ft")),
            P(("ex", "ft")),
            P(None, ("ex", "ft")),
            P(None, ("ex", "ft")),
        ),
        out_specs=(P(("ex", "ft")), P(("ex", "ft"))),
        check_vma=False,
    )
```

```python
import functools

import jax
import jax.numpy as jnp
from jax import lax
from jax.experimental import pallas as pl
from jax.experimental.pallas import tpu as pltpu
from jax.sharding import PartitionSpec as P

ITERS = 2
LANES = 128
MESH = pl.DeviceIdType.MESH
HIGH = lax.Precision.HIGHEST


GROUPS = 4


def kernel(ne, nf, features, labels_hbm, weights, hist_s, hist_y, new_weights, direction,
           feat, s, y, labels, wbf, wf, wg, sib_out, sib_in, own, chip_out, chip_in,
           grads, rows_out, rows_in, bf_out, bf_in, ac, bc, atc,
           feat_sem, hist_sem, ag_send, ag_recv, fw_send, fw_recv,
           sb_send, sb_recv, cp_send, cp_recv, ar_send, ar_recv, bf_send, bf_recv):
    nd = ne * nf
    chips = nd // 2
    examples = features.shape[0]
    rows = weights.shape[0]
    pairs = hist_s.shape[0]
    f32, bf16 = jnp.float32, jnp.bfloat16
    me = lax.axis_index("ex") * nf + lax.axis_index("ft")
    chip, core = me // 2, me % 2
    sibling = 2 * chip + (1 - core)

    def at(device):
        return (device // nf, device % nf)

    def remote(src, dst, send, recv, device):
        return pltpu.make_async_remote_copy(
            src_ref=src, dst_ref=dst, send_sem=send, recv_sem=recv,
            device_id=at(device), device_id_type=MESH)

    barrier = pltpu.get_barrier_semaphore()

    def greet(k, carry):
        pl.semaphore_signal(barrier, inc=1, device_id=at((me + k) % nd), device_id_type=MESH)
        return carry

    lax.fori_loop(1, nd, greet, 0)

    parts = feat_sem.shape[0]
    width = features.shape[1] // parts
    loads = [pltpu.make_async_copy(features.at[:, pl.ds(i * width, width)],
                                   feat.at[:, pl.ds(i * width, width)], feat_sem.at[i])
             for i in range(parts)]
    hist_loads = [pltpu.make_async_copy(hist_s, s, hist_sem.at[0]),
                  pltpu.make_async_copy(hist_y, y, hist_sem.at[1])]
    small_loads = [pltpu.make_async_copy(weights, wf.at[0], hist_sem.at[2]),
                   pltpu.make_async_copy(labels_hbm, labels, hist_sem.at[3])]
    for copy in small_loads + hist_loads + loads:
        copy.start()
    for copy in small_loads:
        copy.wait()
    wbf[0] = wf[0].astype(bf16)
    wg[0, core, 0] = wf[0].astype(bf16)
    pl.semaphore_wait(barrier, nd - 1)

    def ag_copy(it, k):
        return remote(wbf.at[it], wg.at[it, core, k], ag_send.at[it], ag_recv.at[it],
                      2 * ((chip + k) % chips) + core)

    def ag_all(it):
        slots = wg.at[it, core, pl.ds(1, chips - 1)]
        return remote(slots, slots, ag_send.at[it], ag_recv.at[it], sibling)

    def fw_copy(it):
        return remote(wg.at[it, core], wg.at[it, core], fw_send.at[it], fw_recv.at[it], sibling)

    def fw_wait(it):
        return remote(wg.at[it, core], wg.at[it, 1 - core], fw_send.at[it], fw_recv.at[it],
                      sibling)

    def gather_start(it):
        def go(k, carry):
            ag_copy(it, k).start()
            return carry

        lax.fori_loop(1, chips, go, 0)

    def dot_block(it, half_chip, k, acc):
        device = 2 * ((chip - k + chips) % chips) + half_chip
        for half in range(rows // 16):
            w16 = wg[it, half_chip, k, pl.ds(half * 16, 16), :].astype(f32)
            start = pl.multiple_of((device * rows + half * 16) * LANES, 16 * LANES)
            tile = feat[:, pl.ds(start, 16 * LANES)]
            for r in range(16):
                acc = acc + tile[:, r * LANES:(r + 1) * LANES].astype(f32) * w16[r:r + 1, :]
        return acc

    bits = bf_out.shape[0] - 1

    def bf_copy(b):
        step = 2 ** b
        partner = me + step * (1 - 2 * ((me // step) % 2))
        return remote(bf_out.at[b], bf_in.at[b], bf_send.at[b], bf_recv.at[b], partner)

    progress = [0]

    def advance():
        b = progress[0]
        if b < bits:
            bf_copy(b).wait()
            bf_out[b + 1] = bf_out[b] + bf_in[b]
            if b + 1 < bits:
                bf_copy(b + 1).start()
            progress[0] = b + 1

    sub = lax.broadcasted_iota(jnp.int32, (pairs, LANES), 0)
    lane = lax.broadcasted_iota(jnp.int32, (pairs, LANES), 1)

    def to_row(acc, offset):
        col = jnp.sum(acc, axis=1, keepdims=True)
        return jnp.sum(jnp.where(lane == sub + offset, col, 0.0), axis=0, keepdims=True)

    def to_col(row, offset):
        col = jnp.sum(jnp.where(lane == sub + offset, row, 0.0), axis=1, keepdims=True)
        return jnp.broadcast_to(col, (pairs, LANES))

    def all_sub(col):
        return jnp.broadcast_to(jnp.sum(col, axis=0, keepdims=True), (pairs, LANES))

    def spread(col, k):
        return jnp.broadcast_to(col[k:k + 1, :], (pairs, LANES))

    def ar_copy(it, k):
        return remote(rows_out.at[it], rows_in.at[it, k], ar_send.at[it], ar_recv.at[it],
                      (me + k) % nd)

    def ar_all(it):
        slots = rows_in.at[it, pl.ds(1, nd - 1)]
        return remote(slots, slots, ar_send.at[it], ar_recv.at[it], sibling)

    gather_start(0)
    hist_loads[0].wait()
    hist_loads[1].wait()

    chunk = min(1024, rows * LANES)
    contract = (((1,), (1,)), ((), ()))

    def products(i, sums):
        a = s[:, pl.ds(pl.multiple_of(i * chunk, chunk), chunk)]
        b = y[:, pl.ds(pl.multiple_of(i * chunk, chunk), chunk)]
        dot = functools.partial(lax.dot_general, dimension_numbers=contract, precision=HIGH,
                                preferred_element_type=f32)
        return (sums[0] + dot(a, b), sums[1] + dot(b, a), sums[2] + dot(b, b))

    zero = jnp.zeros((pairs, pairs), f32)
    sy, ys, yy = lax.fori_loop(0, rows * LANES // chunk, products, (zero, zero, zero))
    pad = jnp.zeros((pairs, LANES - 3 * pairs), f32)
    bf_out[0] = jnp.concatenate([sy, ys, yy, pad], axis=1)
    bf_copy(0).start()
    for copy in loads:
        copy.wait()

    for it in range(ITERS):
        if it > 0:
            wf[ITERS + it] = wf[it] - wf[it - 1]
            for r in range(rows):
                s[0:1, r * LANES:(r + 1) * LANES] = wf[ITERS + it, r:r + 1, :]
        ag_all(it).wait_recv()
        fw_copy(it).start()
        advance()
        acc = lax.fori_loop(0, chips, lambda k, acc: dot_block(it, core, k, acc),
                            jnp.zeros((examples, LANES), f32))
        fw_wait(it).wait_recv()
        acc = lax.fori_loop(0, chips, lambda k, acc: dot_block(it, 1 - core, k, acc), acc)
        advance()
        margin = jnp.sum(acc, axis=1, keepdims=True)
        wide = 16 * examples
        on_diag = (lax.broadcasted_iota(jnp.int32, (examples, examples), 0)
                   == lax.broadcasted_iota(jnp.int32, (examples, examples), 1))
        label = jnp.sum(jnp.where(on_diag, labels[...].astype(f32), 0.0), axis=1, keepdims=True)
        resid = (1.0 / (1.0 + jnp.exp(-margin)) - label).astype(bf16).astype(f32)
        esub = lax.broadcasted_iota(jnp.int32, (examples, wide), 0)
        elane = lax.broadcasted_iota(jnp.int32, (examples, wide), 1)
        flat = jnp.sum(jnp.where(elane % examples == esub, resid, 0.0), axis=0, keepdims=True)
        gsub = lax.broadcasted_iota(jnp.int32, (16, wide), 0)
        glane = lax.broadcasted_iota(jnp.int32, (16, wide), 1)
        select = jnp.where(glane // examples == gsub, flat, 0.0).astype(bf16)

        def terms(device, part):
            start = pl.multiple_of((device * rows + part * 16) * LANES, 16 * LANES)
            tile = feat[:, pl.ds(start, 16 * LANES)]
            stack = jnp.concatenate(
                [tile[:, r * LANES:(r + 1) * LANES] for r in range(16)], axis=0)
            return jnp.dot(select, stack, preferred_element_type=f32)

        per = chips // GROUPS

        def sb_copy(g):
            slots = pl.ds(g * per, per)
            return remote(sib_out.at[it, slots], sib_in.at[it, slots], sb_send.at[it, g],
                          sb_recv.at[it, g], sibling)

        def cp_copy(k):
            return remote(chip_out.at[it, k], chip_in.at[it, k], cp_send.at[it],
                          cp_recv.at[it], 2 * ((chip + k) % chips) + core)

        def cp_all():
            slots = chip_in.at[it, pl.ds(1, chips - 1)]
            return remote(slots, slots, cp_send.at[it], cp_recv.at[it], sibling)

        def compute(k, carry):
            target = 2 * ((chip + k) % chips)
            for part in range(rows // 16):
                sib_out[it, k, pl.ds(part * 16, 16), :] = terms(target + 1 - core, part)
                own[k, pl.ds(part * 16, 16), :] = terms(target + core, part)
            return carry

        def relay(k, carry):
            chip_out[it, k] = (own[k] + sib_in[it, k]).astype(bf16)
            cp_copy(k).start()
            return carry

        def relay_group(g):
            sb_copy(g).wait_recv()
            lax.fori_loop(max(1, g * per), (g + 1) * per, relay, 0)

        order = list(reversed(range(GROUPS)))
        for i, g in enumerate(order):
            lax.fori_loop(g * per, (g + 1) * per, compute, 0)
            sb_copy(g).start()
            if i > 0:
                relay_group(order[i - 1])
        relay_group(order[-1])
        advance()
        total = own[0] + sib_in[it, 0]
        cp_all().wait_recv()
        total = lax.fori_loop(
            1, chips, lambda k, total: total + chip_in[it, k].astype(f32), total)
        advance()
        w = wf[it]
        grad = total + 0.1 * w
        grads[it] = grad

        if it > 0:
            grads[ITERS + it] = grad - grads[it - 1]
            for r in range(rows):
                y[0:1, r * LANES:(r + 1) * LANES] = grads[ITERS + it, r:r + 1, :]
        accs = [jnp.zeros((pairs, LANES), f32) for _ in range(4 if it > 0 else 2)]
        for r in range(rows):
            st = s[:, r * LANES:(r + 1) * LANES]
            yt = y[:, r * LANES:(r + 1) * LANES]
            g = grads[it, r:r + 1, :]
            accs[0] = accs[0] + st * g
            accs[1] = accs[1] + yt * g
            if it > 0:
                dg = grads[ITERS + it, r:r + 1, :]
                accs[2] = accs[2] + st * dg
                accs[3] = accs[3] + yt * dg
        packed = to_row(accs[0], 0)
        for i in range(1, len(accs)):
            packed = packed + to_row(accs[i], i * pairs)
        rows_out[it] = packed
        rows_in[it, 0] = packed

        def ar_start(k, carry):
            ar_copy(it, k).start()
            return carry

        lax.fori_loop(1, nd, ar_start, 0)
        if it == 0:
            while progress[0] < bits:
                advance()
            gram = bf_out[bits]
            diag = to_col(gram, 0)
            dinv = 1.0 / diag
            for k in range(pairs):
                col = jnp.broadcast_to(gram[:, k:k + 1], (pairs, LANES))
                ac[k] = jnp.where(sub < k, col * dinv, 0.0)
                col = jnp.broadcast_to(gram[:, pairs + k:pairs + k + 1], (pairs, LANES))
                atc[k] = jnp.where(sub > k, col * dinv, 0.0)
                bc[k] = jnp.broadcast_to(gram[:, 2 * pairs + k:2 * pairs + k + 1], (pairs, LANES))
            last = pairs - 1
            gamma = spread(diag, last) / spread(bc[last], last)
        ar_all(it).wait_recv()
        summed = jnp.sum(rows_in[it], axis=0)
        p, q = to_col(summed, 0), to_col(summed, pairs)

        first = sub == 0
        if it > 0:
            sdy, ydy = to_col(summed, 2 * pairs), to_col(summed, 3 * pairs)
            diag = jnp.where(first, sdy, diag)
            dinv = 1.0 / diag
            gamma = spread(sdy, 0) / spread(ydy, 0)
        t, v = -p * dinv, q
        if it > 0:
            a = spread(t, 0)
            t = t - a * jnp.where(first, 0.0, sdy * dinv)
            v = v + a * ydy
        for k in reversed(range(min(it, 1), pairs)):
            a = spread(t, k)
            column = ac[k]
            if it > 0:
                column = jnp.where(first, 0.0, column)
            t = t - a * column
            v = v + a * bc[k]
        if it > 0:
            v = jnp.where(first, q + all_sub(t * ydy), v)
        u = t + gamma * v * dinv
        for k in range(min(it, 1), pairs):
            u = u - spread(u, k) * atc[k]
        if it > 0:
            u = jnp.where(first, u - all_sub(jnp.where(first, 0.0, u * sdy)) * dinv, u)
        cy = -gamma * t
        cg = gamma[0:1, :]
        for r in range(rows):
            st = s[:, r * LANES:(r + 1) * LANES]
            yt = y[:, r * LANES:(r + 1) * LANES]
            step = jnp.sum(st * u + yt * cy, axis=0, keepdims=True) - cg * grads[it, r:r + 1, :]
            grads[ITERS, r:r + 1, :] = step
        w = w + grads[ITERS]
        if it + 1 < ITERS:
            wf[it + 1] = w
            wbf[it + 1] = w.astype(bf16)
            wg[it + 1, core, 0] = w.astype(bf16)
            gather_start(it + 1)
        else:
            new_weights[...] = w
            direction[...] = grads[ITERS]

        ag_all(it).wait_send()
        fw_copy(it).wait_send()
        cp_all().wait_send()
        ar_all(it).wait_send()
        for g in range(GROUPS):
            sb_copy(g).wait_send()


def finish(w, d, w_out, d_out):
    w_out[...] = w[...]
    d_out[...] = d[...]


def per_device(ne, nf, features, labels, start_weights, hist_s, hist_y):
    nd = ne * nf
    chips = nd // 2
    bits = nd.bit_length() - 1
    examples = features.shape[0]
    size = start_weights.shape[0]
    pairs = hist_s.shape[0]
    rows = size // LANES
    f32, bf16 = jnp.float32, jnp.bfloat16
    vmem, dma = pltpu.VMEM, pltpu.SemaphoreType.DMA
    block = jax.ShapeDtypeStruct((rows, LANES), f32)
    in_vmem = pl.BlockSpec(memory_space=pltpu.VMEM)
    in_hbm = pl.BlockSpec(memory_space=pl.ANY)
    out = pl.pallas_call(
        functools.partial(kernel, ne, nf),
        out_shape=(block, block),
        in_specs=[in_hbm] * 5,
        out_specs=(in_vmem, in_vmem),
        scratch_shapes=[
            vmem(features.shape, bf16),
            vmem(hist_s.shape, f32),
            vmem(hist_y.shape, f32),
            vmem((1, examples), jnp.int32),
            vmem((ITERS, rows, LANES), bf16),
            vmem((2 * ITERS, rows, LANES), f32),
            vmem((ITERS, 2, chips, rows, LANES), bf16),
            vmem((ITERS, chips, rows, LANES), f32),
            vmem((ITERS, chips, rows, LANES), f32),
            vmem((chips, rows, LANES), f32),
            vmem((ITERS, chips, rows, LANES), bf16),
            vmem((ITERS, chips, rows, LANES), bf16),
            vmem((2 * ITERS, rows, LANES), f32),
            vmem((ITERS, 1, LANES), f32),
            vmem((ITERS, nd, 1, LANES), f32),
            vmem((bits + 1, pairs, LANES), f32),
            vmem((bits, pairs, LANES), f32),
            vmem((pairs, pairs, LANES), f32),
            vmem((pairs, pairs, LANES), f32),
            vmem((pairs, pairs, LANES), f32),
            dma((8,)), dma((4,)),
            dma((ITERS,)), dma((ITERS,)),
            dma((ITERS,)), dma((ITERS,)),
            dma((ITERS, GROUPS)), dma((ITERS, GROUPS)),
            dma((ITERS,)), dma((ITERS,)),
            dma((ITERS,)), dma((ITERS,)),
            dma((bits,)), dma((bits,)),
        ],
        compiler_params=pltpu.CompilerParams(collective_id=0, has_side_effects=True),
    )(features, labels.reshape(1, examples), start_weights.reshape(rows, LANES), hist_s, hist_y)
    out = pl.pallas_call(finish, out_shape=(block, block), in_specs=[in_vmem] * 2,
                         out_specs=(in_vmem, in_vmem))(*out)
    return out[0].reshape(size), out[1].reshape(size)


def solution(mesh):
    return jax.shard_map(
        functools.partial(per_device, mesh.shape["ex"], mesh.shape["ft"]),
        mesh=mesh,
        in_specs=(
            P(("ex", "ft"), None),
            P(("ex", "ft")),
            P(("ex", "ft")),
            P(None, ("ex", "ft")),
            P(None, ("ex", "ft")),
        ),
        out_specs=(P(("ex", "ft")), P(("ex", "ft"))),
        check_vma=False,
    )
```

```python
import functools

import jax
import jax.numpy as jnp
from jax import lax
from jax.experimental import pallas as pl
from jax.experimental.pallas import tpu as pltpu
from jax.sharding import PartitionSpec as P

ITERS = 2
LANES = 128
MESH = pl.DeviceIdType.MESH
HIGH = lax.Precision.HIGHEST


GROUPS = 4


def kernel(ne, nf, features, labels_hbm, weights, hist_s, hist_y, new_weights, direction,
           feat, s, y, labels, wbf, wf, wg, sib_out, sib_in, own, chip_out, chip_in,
           grads, rows_out, rows_in, bf_out, bf_in, ac, bc, atc,
           feat_sem, hist_sem, ag_send, ag_recv, fw_send, fw_recv,
           sb_send, sb_recv, cp_send, cp_recv, ar_send, ar_recv, bf_send, bf_recv):
    nd = ne * nf
    chips = nd // 2
    examples = features.shape[0]
    rows = weights.shape[0]
    pairs = hist_s.shape[0]
    f32, bf16 = jnp.float32, jnp.bfloat16
    me = lax.axis_index("ex") * nf + lax.axis_index("ft")
    chip, core = me // 2, me % 2
    sibling = 2 * chip + (1 - core)

    def at(device):
        return (device // nf, device % nf)

    def remote(src, dst, send, recv, device):
        return pltpu.make_async_remote_copy(
            src_ref=src, dst_ref=dst, send_sem=send, recv_sem=recv,
            device_id=at(device), device_id_type=MESH)

    barrier = pltpu.get_barrier_semaphore()

    def greet(k, carry):
        pl.semaphore_signal(barrier, inc=1, device_id=at((me + k) % nd), device_id_type=MESH)
        return carry

    lax.fori_loop(1, nd, greet, 0)

    parts = feat_sem.shape[0]
    width = features.shape[1] // parts
    loads = [pltpu.make_async_copy(features.at[:, pl.ds(i * width, width)],
                                   feat.at[:, pl.ds(i * width, width)], feat_sem.at[i])
             for i in range(parts)]
    hist_loads = [pltpu.make_async_copy(hist_s, s, hist_sem.at[0]),
                  pltpu.make_async_copy(hist_y, y, hist_sem.at[1])]
    small_loads = [pltpu.make_async_copy(weights, wf.at[0], hist_sem.at[2]),
                   pltpu.make_async_copy(labels_hbm, labels, hist_sem.at[3])]
    for copy in small_loads + hist_loads + loads:
        copy.start()
    for copy in small_loads:
        copy.wait()
    wbf[0] = wf[0].astype(bf16)
    wg[0, core, 0] = wf[0].astype(bf16)
    pl.semaphore_wait(barrier, nd - 1)

    per = chips // GROUPS

    def ag_copy(it, k):
        return remote(wbf.at[it], wg.at[it, core, k], ag_send.at[it], ag_recv.at[it, k // per],
                      2 * ((chip + k) % chips) + core)

    def ag_sent(it):
        slots = wg.at[it, core, pl.ds(1, chips - 1)]
        return remote(slots, slots, ag_send.at[it], ag_recv.at[it, 0], sibling)

    def ag_group(it, g):
        first = max(1, g * per)
        slots = wg.at[it, core, pl.ds(first, (g + 1) * per - first)]
        return remote(slots, slots, ag_send.at[it], ag_recv.at[it, g], sibling)

    def fw_copy(it, g, half_chip):
        slots = pl.ds(g * per, per)
        return remote(wg.at[it, core, slots], wg.at[it, half_chip, slots], fw_send.at[it, g],
                      fw_recv.at[it, g], sibling)

    def gather_start(it):
        for k in range(1, chips):
            ag_copy(it, k).start()

    def dot_block(it, half_chip, k, acc):
        device = 2 * ((chip - k + chips) % chips) + half_chip
        for half in range(rows // 16):
            w16 = wg[it, half_chip, k, pl.ds(half * 16, 16), :].astype(f32)
            start = pl.multiple_of((device * rows + half * 16) * LANES, 16 * LANES)
            tile = feat[:, pl.ds(start, 16 * LANES)]
            for r in range(16):
                acc = acc + tile[:, r * LANES:(r + 1) * LANES].astype(f32) * w16[r:r + 1, :]
        return acc

    bits = bf_out.shape[0] - 1

    def bf_copy(b):
        step = 2 ** b
        partner = me + step * (1 - 2 * ((me // step) % 2))
        return remote(bf_out.at[b], bf_in.at[b], bf_send.at[b], bf_recv.at[b], partner)

    progress = [0]

    def advance():
        b = progress[0]
        if b < bits:
            bf_copy(b).wait()
            bf_out[b + 1] = bf_out[b] + bf_in[b]
            if b + 1 < bits:
                bf_copy(b + 1).start()
            progress[0] = b + 1

    sub = lax.broadcasted_iota(jnp.int32, (pairs, LANES), 0)
    lane = lax.broadcasted_iota(jnp.int32, (pairs, LANES), 1)

    def to_row(acc, offset):
        col = jnp.sum(acc, axis=1, keepdims=True)
        return jnp.sum(jnp.where(lane == sub + offset, col, 0.0), axis=0, keepdims=True)

    def to_col(row, offset):
        col = jnp.sum(jnp.where(lane == sub + offset, row, 0.0), axis=1, keepdims=True)
        return jnp.broadcast_to(col, (pairs, LANES))

    def all_sub(col):
        return jnp.broadcast_to(jnp.sum(col, axis=0, keepdims=True), (pairs, LANES))

    def spread(col, k):
        return jnp.broadcast_to(col[k:k + 1, :], (pairs, LANES))

    def ar_copy(it, k):
        return remote(rows_out.at[it], rows_in.at[it, k], ar_send.at[it], ar_recv.at[it],
                      (me + k) % nd)

    def ar_all(it):
        slots = rows_in.at[it, pl.ds(1, nd - 1)]
        return remote(slots, slots, ar_send.at[it], ar_recv.at[it], sibling)

    gather_start(0)
    hist_loads[0].wait()
    hist_loads[1].wait()

    chunk = min(1024, rows * LANES)
    contract = (((1,), (1,)), ((), ()))

    def products(i, sums):
        a = s[:, pl.ds(pl.multiple_of(i * chunk, chunk), chunk)]
        b = y[:, pl.ds(pl.multiple_of(i * chunk, chunk), chunk)]
        dot = functools.partial(lax.dot_general, dimension_numbers=contract, precision=HIGH,
                                preferred_element_type=f32)
        return (sums[0] + dot(a, b), sums[1] + dot(b, a), sums[2] + dot(b, b))

    zero = jnp.zeros((pairs, pairs), f32)
    sy, ys, yy = lax.fori_loop(0, rows * LANES // chunk, products, (zero, zero, zero))
    pad = jnp.zeros((pairs, LANES - 3 * pairs), f32)
    bf_out[0] = jnp.concatenate([sy, ys, yy, pad], axis=1)
    bf_copy(0).start()

    for it in range(ITERS):
        if it > 0:
            wf[ITERS + it] = wf[it] - wf[it - 1]
            for r in range(rows):
                s[0:1, r * LANES:(r + 1) * LANES] = wf[ITERS + it, r:r + 1, :]
        acc = jnp.zeros((examples, LANES), f32)

        def margins(g, half_chip, acc):
            return lax.fori_loop(g * per, (g + 1) * per,
                                 lambda k, acc: dot_block(it, half_chip, k, acc), acc)

        for g in range(GROUPS):
            if per > 1 or g > 0:
                ag_group(it, g).wait_recv()
            fw_copy(it, g, core).start()
            if it == 0 and g == 0:
                for copy in loads:
                    copy.wait()
            acc = margins(g, core, acc)
            if g > 0:
                fw_copy(it, g - 1, 1 - core).wait_recv()
                acc = margins(g - 1, 1 - core, acc)
            if g % 2 == 1:
                advance()
        fw_copy(it, GROUPS - 1, 1 - core).wait_recv()
        acc = margins(GROUPS - 1, 1 - core, acc)
        advance()
        margin = jnp.sum(acc, axis=1, keepdims=True)
        wide = 16 * examples
        on_diag = (lax.broadcasted_iota(jnp.int32, (examples, examples), 0)
                   == lax.broadcasted_iota(jnp.int32, (examples, examples), 1))
        label = jnp.sum(jnp.where(on_diag, labels[...].astype(f32), 0.0), axis=1, keepdims=True)
        resid = (1.0 / (1.0 + jnp.exp(-margin)) - label).astype(bf16).astype(f32)
        esub = lax.broadcasted_iota(jnp.int32, (examples, wide), 0)
        elane = lax.broadcasted_iota(jnp.int32, (examples, wide), 1)
        flat = jnp.sum(jnp.where(elane % examples == esub, resid, 0.0), axis=0, keepdims=True)
        gsub = lax.broadcasted_iota(jnp.int32, (16, wide), 0)
        glane = lax.broadcasted_iota(jnp.int32, (16, wide), 1)
        select = jnp.where(glane // examples == gsub, flat, 0.0).astype(bf16)

        def terms(device, part):
            start = pl.multiple_of((device * rows + part * 16) * LANES, 16 * LANES)
            tile = feat[:, pl.ds(start, 16 * LANES)]
            stack = jnp.concatenate(
                [tile[:, r * LANES:(r + 1) * LANES] for r in range(16)], axis=0)
            return jnp.dot(select, stack, preferred_element_type=f32)

        def sb_copy(g):
            slots = pl.ds(g * per, per)
            return remote(sib_out.at[it, slots], sib_in.at[it, slots], sb_send.at[it, g],
                          sb_recv.at[it, g], sibling)

        def cp_copy(k):
            return remote(chip_out.at[it, k], chip_in.at[it, k], cp_send.at[it],
                          cp_recv.at[it], 2 * ((chip + k) % chips) + core)

        def cp_all():
            slots = chip_in.at[it, pl.ds(1, chips - 1)]
            return remote(slots, slots, cp_send.at[it], cp_recv.at[it], sibling)

        def compute(k, carry):
            target = 2 * ((chip + k) % chips)
            for part in range(rows // 16):
                sib_out[it, k, pl.ds(part * 16, 16), :] = terms(target + 1 - core, part)
                own[k, pl.ds(part * 16, 16), :] = terms(target + core, part)
            return carry

        def relay(k, carry):
            chip_out[it, k] = (own[k] + sib_in[it, k]).astype(bf16)
            cp_copy(k).start()
            return carry

        def relay_group(g):
            sb_copy(g).wait_recv()
            lax.fori_loop(max(1, g * per), (g + 1) * per, relay, 0)

        order = list(reversed(range(GROUPS)))
        for i, g in enumerate(order):
            lax.fori_loop(g * per, (g + 1) * per, compute, 0)
            sb_copy(g).start()
            if i > 0:
                relay_group(order[i - 1])
        relay_group(order[-1])
        advance()
        total = own[0] + sib_in[it, 0]
        cp_all().wait_recv()
        total = lax.fori_loop(
            1, chips, lambda k, total: total + chip_in[it, k].astype(f32), total)
        advance()
        w = wf[it]
        grad = total + 0.1 * w
        grads[it] = grad

        if it > 0:
            grads[ITERS + it] = grad - grads[it - 1]
            for r in range(rows):
                y[0:1, r * LANES:(r + 1) * LANES] = grads[ITERS + it, r:r + 1, :]
        accs = [jnp.zeros((pairs, LANES), f32) for _ in range(4 if it > 0 else 2)]
        for r in range(rows):
            st = s[:, r * LANES:(r + 1) * LANES]
            yt = y[:, r * LANES:(r + 1) * LANES]
            g = grads[it, r:r + 1, :]
            accs[0] = accs[0] + st * g
            accs[1] = accs[1] + yt * g
            if it > 0:
                dg = grads[ITERS + it, r:r + 1, :]
                accs[2] = accs[2] + st * dg
                accs[3] = accs[3] + yt * dg
        packed = to_row(accs[0], 0)
        for i in range(1, len(accs)):
            packed = packed + to_row(accs[i], i * pairs)
        rows_out[it] = packed
        rows_in[it, 0] = packed

        def ar_start(k, carry):
            ar_copy(it, k).start()
            return carry

        if nd <= 32:
            for k in range(1, nd):
                ar_copy(it, k).start()
        else:
            lax.fori_loop(1, nd, ar_start, 0)
        if it == 0:
            while progress[0] < bits:
                advance()
            gram = bf_out[bits]
            diag = to_col(gram, 0)
            dinv = 1.0 / diag
            for k in range(pairs):
                col = jnp.broadcast_to(gram[:, k:k + 1], (pairs, LANES))
                ac[k] = jnp.where(sub < k, col * dinv, 0.0)
                col = jnp.broadcast_to(gram[:, pairs + k:pairs + k + 1], (pairs, LANES))
                atc[k] = jnp.where(sub > k, col * dinv, 0.0)
                bc[k] = jnp.broadcast_to(gram[:, 2 * pairs + k:2 * pairs + k + 1], (pairs, LANES))
            last = pairs - 1
            gamma = spread(diag, last) / spread(bc[last], last)
        ar_all(it).wait_recv()
        summed = jnp.sum(rows_in[it], axis=0)
        p, q = to_col(summed, 0), to_col(summed, pairs)

        first = sub == 0
        if it > 0:
            sdy, ydy = to_col(summed, 2 * pairs), to_col(summed, 3 * pairs)
            diag = jnp.where(first, sdy, diag)
            dinv = 1.0 / diag
            gamma = spread(sdy, 0) / spread(ydy, 0)
        t, v = -p * dinv, q
        if it > 0:
            a = spread(t, 0)
            t = t - a * jnp.where(first, 0.0, sdy * dinv)
            v = v + a * ydy
        for k in reversed(range(min(it, 1), pairs)):
            a = spread(t, k)
            column = ac[k]
            if it > 0:
                column = jnp.where(first, 0.0, column)
            t = t - a * column
            v = v + a * bc[k]
        if it > 0:
            v = jnp.where(first, q + all_sub(t * ydy), v)
        u = t + gamma * v * dinv
        for k in range(min(it, 1), pairs):
            u = u - spread(u, k) * atc[k]
        if it > 0:
            u = jnp.where(first, u - all_sub(jnp.where(first, 0.0, u * sdy)) * dinv, u)
        cy = -gamma * t
        cg = gamma[0:1, :]
        for r in range(rows):
            st = s[:, r * LANES:(r + 1) * LANES]
            yt = y[:, r * LANES:(r + 1) * LANES]
            step = jnp.sum(st * u + yt * cy, axis=0, keepdims=True) - cg * grads[it, r:r + 1, :]
            grads[ITERS, r:r + 1, :] = step
        w = w + grads[ITERS]
        if it + 1 < ITERS:
            wf[it + 1] = w
            wbf[it + 1] = w.astype(bf16)
            wg[it + 1, core, 0] = w.astype(bf16)
            gather_start(it + 1)
        else:
            new_weights[...] = w
            direction[...] = grads[ITERS]

        ag_sent(it).wait_send()
        cp_all().wait_send()
        ar_all(it).wait_send()
        for g in range(GROUPS):
            fw_copy(it, g, core).wait_send()
            sb_copy(g).wait_send()


def finish(w, d, w_out, d_out):
    w_out[...] = w[...]
    d_out[...] = d[...]


def per_device(ne, nf, features, labels, start_weights, hist_s, hist_y):
    nd = ne * nf
    chips = nd // 2
    bits = nd.bit_length() - 1
    examples = features.shape[0]
    size = start_weights.shape[0]
    pairs = hist_s.shape[0]
    rows = size // LANES
    f32, bf16 = jnp.float32, jnp.bfloat16
    vmem, dma = pltpu.VMEM, pltpu.SemaphoreType.DMA
    block = jax.ShapeDtypeStruct((rows, LANES), f32)
    in_vmem = pl.BlockSpec(memory_space=pltpu.VMEM)
    in_hbm = pl.BlockSpec(memory_space=pl.ANY)
    out = pl.pallas_call(
        functools.partial(kernel, ne, nf),
        out_shape=(block, block),
        in_specs=[in_hbm] * 5,
        out_specs=(in_vmem, in_vmem),
        scratch_shapes=[
            vmem(features.shape, bf16),
            vmem(hist_s.shape, f32),
            vmem(hist_y.shape, f32),
            vmem((1, examples), jnp.int32),
            vmem((ITERS, rows, LANES), bf16),
            vmem((2 * ITERS, rows, LANES), f32),
            vmem((ITERS, 2, chips, rows, LANES), bf16),
            vmem((ITERS, chips, rows, LANES), f32),
            vmem((ITERS, chips, rows, LANES), f32),
            vmem((chips, rows, LANES), f32),
            vmem((ITERS, chips, rows, LANES), bf16),
            vmem((ITERS, chips, rows, LANES), bf16),
            vmem((2 * ITERS, rows, LANES), f32),
            vmem((ITERS, 1, LANES), f32),
            vmem((ITERS, nd, 1, LANES), f32),
            vmem((bits + 1, pairs, LANES), f32),
            vmem((bits, pairs, LANES), f32),
            vmem((pairs, pairs, LANES), f32),
            vmem((pairs, pairs, LANES), f32),
            vmem((pairs, pairs, LANES), f32),
            dma((8,)), dma((4,)),
            dma((ITERS,)), dma((ITERS, GROUPS)),
            dma((ITERS, GROUPS)), dma((ITERS, GROUPS)),
            dma((ITERS, GROUPS)), dma((ITERS, GROUPS)),
            dma((ITERS,)), dma((ITERS,)),
            dma((ITERS,)), dma((ITERS,)),
            dma((bits,)), dma((bits,)),
        ],
        compiler_params=pltpu.CompilerParams(collective_id=0, has_side_effects=True),
    )(features, labels.reshape(1, examples), start_weights.reshape(rows, LANES), hist_s, hist_y)
    out = pl.pallas_call(finish, out_shape=(block, block), in_specs=[in_vmem] * 2,
                         out_specs=(in_vmem, in_vmem))(*out)
    return out[0].reshape(size), out[1].reshape(size)


def solution(mesh):
    return jax.shard_map(
        functools.partial(per_device, mesh.shape["ex"], mesh.shape["ft"]),
        mesh=mesh,
        in_specs=(
            P(("ex", "ft"), None),
            P(("ex", "ft")),
            P(("ex", "ft")),
            P(None, ("ex", "ft")),
            P(None, ("ex", "ft")),
        ),
        out_specs=(P(("ex", "ft")), P(("ex", "ft"))),
        check_vma=False,
    )
```

```python
import functools

import jax
import jax.numpy as jnp
from jax import lax
from jax.experimental import pallas as pl
from jax.experimental.pallas import tpu as pltpu
from jax.sharding import PartitionSpec as P

ITERS = 2
LANES = 128
MESH = pl.DeviceIdType.MESH
HIGH = lax.Precision.HIGHEST


GROUPS = 4


def kernel(ne, nf, features, labels_hbm, weights, hist_s, hist_y, new_weights, direction,
           feat, s, y, labels, wbf, wf, wg, sib_out, sib_in, own, chip_out, chip_in,
           grads, rows_out, rows_in, bf_out, bf_in, ac, bc, atc,
           feat_sem, hist_sem, ag_send, ag_recv, fw_send, fw_recv,
           sb_send, sb_recv, cp_send, cp_recv, ar_send, ar_recv, bf_send, bf_recv):
    nd = ne * nf
    chips = nd // 2
    examples = features.shape[0]
    rows = weights.shape[0]
    pairs = hist_s.shape[0]
    f32, bf16 = jnp.float32, jnp.bfloat16
    me = lax.axis_index("ex") * nf + lax.axis_index("ft")
    chip, core = me // 2, me % 2
    sibling = 2 * chip + (1 - core)

    def flip(place, k, count):
        bits = [2 ** i for i in range(count.bit_length() - 1)]
        return sum(((place // b + k // b) % 2) * b for b in bits)

    def mate(k):
        return flip(chip, k, chips)

    def at(device):
        return (device // nf, device % nf)

    def remote(src, dst, send, recv, device):
        return pltpu.make_async_remote_copy(
            src_ref=src, dst_ref=dst, send_sem=send, recv_sem=recv,
            device_id=at(device), device_id_type=MESH)

    barrier = pltpu.get_barrier_semaphore()

    def greet(k, carry):
        pl.semaphore_signal(barrier, inc=1, device_id=at((me + k) % nd), device_id_type=MESH)
        return carry

    lax.fori_loop(1, nd, greet, 0)

    parts = feat_sem.shape[0]
    width = features.shape[1] // parts
    loads = [pltpu.make_async_copy(features.at[:, pl.ds(i * width, width)],
                                   feat.at[:, pl.ds(i * width, width)], feat_sem.at[i])
             for i in range(parts)]
    hist_loads = [pltpu.make_async_copy(hist_s, s, hist_sem.at[0]),
                  pltpu.make_async_copy(hist_y, y, hist_sem.at[1])]
    small_loads = [pltpu.make_async_copy(weights, wf.at[0], hist_sem.at[2]),
                   pltpu.make_async_copy(labels_hbm, labels, hist_sem.at[3])]
    for copy in small_loads + hist_loads + loads:
        copy.start()
    for copy in small_loads:
        copy.wait()
    wbf[0] = wf[0].astype(bf16)
    wg[0, core, 0] = wf[0].astype(bf16)
    pl.semaphore_wait(barrier, nd - 1)

    per = chips // GROUPS

    def ag_copy(it, k):
        return remote(wbf.at[it], wg.at[it, core, k], ag_send.at[it], ag_recv.at[it, k // per],
                      2 * mate(k) + core)

    def ag_sent(it):
        slots = wg.at[it, core, pl.ds(1, chips - 1)]
        return remote(slots, slots, ag_send.at[it], ag_recv.at[it, 0], sibling)

    def ag_group(it, g):
        first = max(1, g * per)
        slots = wg.at[it, core, pl.ds(first, (g + 1) * per - first)]
        return remote(slots, slots, ag_send.at[it], ag_recv.at[it, g], sibling)

    def fw_copy(it, g, half_chip):
        slots = pl.ds(g * per, per)
        return remote(wg.at[it, core, slots], wg.at[it, half_chip, slots], fw_send.at[it, g],
                      fw_recv.at[it, g], sibling)

    def gather_start(it):
        for k in reversed(range(1, chips)):
            ag_copy(it, k).start()

    def dot_block(it, half_chip, k, acc):
        device = 2 * mate(k) + half_chip
        for half in range(rows // 16):
            w16 = wg[it, half_chip, k, pl.ds(half * 16, 16), :].astype(f32)
            start = pl.multiple_of((device * rows + half * 16) * LANES, 16 * LANES)
            tile = feat[:, pl.ds(start, 16 * LANES)]
            for r in range(16):
                acc = acc + tile[:, r * LANES:(r + 1) * LANES].astype(f32) * w16[r:r + 1, :]
        return acc

    bits = bf_out.shape[0] - 1

    def bf_copy(b):
        step = 2 ** b
        partner = me + step * (1 - 2 * ((me // step) % 2))
        return remote(bf_out.at[b], bf_in.at[b], bf_send.at[b], bf_recv.at[b], partner)

    progress = [0]

    def advance():
        b = progress[0]
        if b < bits:
            bf_copy(b).wait()
            bf_out[b + 1] = bf_out[b] + bf_in[b]
            if b + 1 < bits:
                bf_copy(b + 1).start()
            progress[0] = b + 1

    sub = lax.broadcasted_iota(jnp.int32, (pairs, LANES), 0)
    lane = lax.broadcasted_iota(jnp.int32, (pairs, LANES), 1)

    def to_row(acc, offset):
        col = jnp.sum(acc, axis=1, keepdims=True)
        return jnp.sum(jnp.where(lane == sub + offset, col, 0.0), axis=0, keepdims=True)

    def to_col(row, offset):
        col = jnp.sum(jnp.where(lane == sub + offset, row, 0.0), axis=1, keepdims=True)
        return jnp.broadcast_to(col, (pairs, LANES))

    def all_sub(col):
        return jnp.broadcast_to(jnp.sum(col, axis=0, keepdims=True), (pairs, LANES))

    def spread(col, k):
        return jnp.broadcast_to(col[k:k + 1, :], (pairs, LANES))

    def ar_copy(it, k):
        return remote(rows_out.at[it], rows_in.at[it, k], ar_send.at[it], ar_recv.at[it],
                      flip(me, k, nd))

    def ar_all(it):
        slots = rows_in.at[it, pl.ds(1, nd - 1)]
        return remote(slots, slots, ar_send.at[it], ar_recv.at[it], sibling)

    gather_start(0)
    hist_loads[0].wait()
    hist_loads[1].wait()

    chunk = min(1024, rows * LANES)
    contract = (((1,), (1,)), ((), ()))

    def products(i, sums):
        a = s[:, pl.ds(pl.multiple_of(i * chunk, chunk), chunk)]
        b = y[:, pl.ds(pl.multiple_of(i * chunk, chunk), chunk)]
        dot = functools.partial(lax.dot_general, dimension_numbers=contract, precision=HIGH,
                                preferred_element_type=f32)
        return (sums[0] + dot(a, b), sums[1] + dot(b, a), sums[2] + dot(b, b))

    zero = jnp.zeros((pairs, pairs), f32)
    sy, ys, yy = lax.fori_loop(0, rows * LANES // chunk, products, (zero, zero, zero))
    pad = jnp.zeros((pairs, LANES - 3 * pairs), f32)
    bf_out[0] = jnp.concatenate([sy, ys, yy, pad], axis=1)
    bf_copy(0).start()

    for it in range(ITERS):
        if it > 0:
            wf[ITERS + it] = wf[it] - wf[it - 1]
            for r in range(rows):
                s[0:1, r * LANES:(r + 1) * LANES] = wf[ITERS + it, r:r + 1, :]
        acc = jnp.zeros((examples, LANES), f32)

        def margins(g, half_chip, acc):
            return lax.fori_loop(g * per, (g + 1) * per,
                                 lambda k, acc: dot_block(it, half_chip, k, acc), acc)

        order = list(reversed(range(GROUPS)))
        for i, g in enumerate(order):
            if per > 1 or g > 0:
                ag_group(it, g).wait_recv()
            fw_copy(it, g, core).start()
            if it == 0 and i == 0:
                for copy in loads:
                    copy.wait()
            acc = margins(g, core, acc)
            if i > 0:
                fw_copy(it, order[i - 1], 1 - core).wait_recv()
                acc = margins(order[i - 1], 1 - core, acc)
            if i % 2 == 1:
                advance()
        fw_copy(it, order[-1], 1 - core).wait_recv()
        acc = margins(order[-1], 1 - core, acc)
        advance()
        margin = jnp.sum(acc, axis=1, keepdims=True)
        wide = 16 * examples
        on_diag = (lax.broadcasted_iota(jnp.int32, (examples, examples), 0)
                   == lax.broadcasted_iota(jnp.int32, (examples, examples), 1))
        label = jnp.sum(jnp.where(on_diag, labels[...].astype(f32), 0.0), axis=1, keepdims=True)
        resid = (1.0 / (1.0 + jnp.exp(-margin)) - label).astype(bf16).astype(f32)
        esub = lax.broadcasted_iota(jnp.int32, (examples, wide), 0)
        elane = lax.broadcasted_iota(jnp.int32, (examples, wide), 1)
        flat = jnp.sum(jnp.where(elane % examples == esub, resid, 0.0), axis=0, keepdims=True)
        gsub = lax.broadcasted_iota(jnp.int32, (16, wide), 0)
        glane = lax.broadcasted_iota(jnp.int32, (16, wide), 1)
        select = jnp.where(glane // examples == gsub, flat, 0.0).astype(bf16)

        def terms(device, part):
            start = pl.multiple_of((device * rows + part * 16) * LANES, 16 * LANES)
            tile = feat[:, pl.ds(start, 16 * LANES)]
            stack = jnp.concatenate(
                [tile[:, r * LANES:(r + 1) * LANES] for r in range(16)], axis=0)
            return jnp.dot(select, stack, preferred_element_type=f32)

        def sb_copy(g):
            slots = pl.ds(g * per, per)
            return remote(sib_out.at[it, slots], sib_in.at[it, slots], sb_send.at[it, g],
                          sb_recv.at[it, g], sibling)

        def cp_copy(k):
            return remote(chip_out.at[it, k], chip_in.at[it, k], cp_send.at[it],
                          cp_recv.at[it], 2 * mate(k) + core)

        def cp_all():
            slots = chip_in.at[it, pl.ds(1, chips - 1)]
            return remote(slots, slots, cp_send.at[it], cp_recv.at[it], sibling)

        def compute(k, carry):
            target = 2 * mate(k)
            for part in range(rows // 16):
                sib_out[it, k, pl.ds(part * 16, 16), :] = terms(target + 1 - core, part)
                own[k, pl.ds(part * 16, 16), :] = terms(target + core, part)
            return carry

        def relay(k, carry):
            chip_out[it, k] = (own[k] + sib_in[it, k]).astype(bf16)
            cp_copy(k).start()
            return carry

        def relay_group(g):
            sb_copy(g).wait_recv()
            lax.fori_loop(max(1, g * per), (g + 1) * per, relay, 0)

        order = list(reversed(range(GROUPS)))
        for i, g in enumerate(order):
            lax.fori_loop(g * per, (g + 1) * per, compute, 0)
            sb_copy(g).start()
            if i > 0:
                relay_group(order[i - 1])
        relay_group(order[-1])
        advance()
        total = own[0] + sib_in[it, 0]
        cp_all().wait_recv()
        total = lax.fori_loop(
            1, chips, lambda k, total: total + chip_in[it, k].astype(f32), total)
        advance()
        w = wf[it]
        grad = total + 0.1 * w
        grads[it] = grad

        if it > 0:
            grads[ITERS + it] = grad - grads[it - 1]
            for r in range(rows):
                y[0:1, r * LANES:(r + 1) * LANES] = grads[ITERS + it, r:r + 1, :]
        accs = [jnp.zeros((pairs, LANES), f32) for _ in range(4 if it > 0 else 2)]
        for r in range(rows):
            st = s[:, r * LANES:(r + 1) * LANES]
            yt = y[:, r * LANES:(r + 1) * LANES]
            g = grads[it, r:r + 1, :]
            accs[0] = accs[0] + st * g
            accs[1] = accs[1] + yt * g
            if it > 0:
                dg = grads[ITERS + it, r:r + 1, :]
                accs[2] = accs[2] + st * dg
                accs[3] = accs[3] + yt * dg
        packed = to_row(accs[0], 0)
        for i in range(1, len(accs)):
            packed = packed + to_row(accs[i], i * pairs)
        rows_out[it] = packed
        rows_in[it, 0] = packed

        def ar_start(k, carry):
            ar_copy(it, k).start()
            return carry

        if nd <= 32:
            for k in reversed(range(1, nd)):
                ar_copy(it, k).start()
        else:
            lax.fori_loop(1, nd, ar_start, 0)
        if it == 0:
            while progress[0] < bits:
                advance()
            gram = bf_out[bits]
            diag = to_col(gram, 0)
            dinv = 1.0 / diag
            for k in range(pairs):
                col = jnp.broadcast_to(gram[:, k:k + 1], (pairs, LANES))
                ac[k] = jnp.where(sub < k, col * dinv, 0.0)
                col = jnp.broadcast_to(gram[:, pairs + k:pairs + k + 1], (pairs, LANES))
                atc[k] = jnp.where(sub > k, col * dinv, 0.0)
                bc[k] = jnp.broadcast_to(gram[:, 2 * pairs + k:2 * pairs + k + 1], (pairs, LANES))
            last = pairs - 1
            gamma = spread(diag, last) / spread(bc[last], last)
        ar_all(it).wait_recv()
        summed = jnp.sum(rows_in[it], axis=0)
        p, q = to_col(summed, 0), to_col(summed, pairs)

        first = sub == 0
        if it > 0:
            sdy, ydy = to_col(summed, 2 * pairs), to_col(summed, 3 * pairs)
            diag = jnp.where(first, sdy, diag)
            dinv = 1.0 / diag
            gamma = spread(sdy, 0) / spread(ydy, 0)
        t, v = -p * dinv, q
        if it > 0:
            a = spread(t, 0)
            t = t - a * jnp.where(first, 0.0, sdy * dinv)
            v = v + a * ydy
        for k in reversed(range(min(it, 1), pairs)):
            a = spread(t, k)
            column = ac[k]
            if it > 0:
                column = jnp.where(first, 0.0, column)
            t = t - a * column
            v = v + a * bc[k]
        if it > 0:
            v = jnp.where(first, q + all_sub(t * ydy), v)
        u = t + gamma * v * dinv
        for k in range(min(it, 1), pairs):
            u = u - spread(u, k) * atc[k]
        if it > 0:
            u = jnp.where(first, u - all_sub(jnp.where(first, 0.0, u * sdy)) * dinv, u)
        cy = -gamma * t
        cg = gamma[0:1, :]
        for r in range(rows):
            st = s[:, r * LANES:(r + 1) * LANES]
            yt = y[:, r * LANES:(r + 1) * LANES]
            step = jnp.sum(st * u + yt * cy, axis=0, keepdims=True) - cg * grads[it, r:r + 1, :]
            grads[ITERS, r:r + 1, :] = step
        w = w + grads[ITERS]
        if it + 1 < ITERS:
            wf[it + 1] = w
            wbf[it + 1] = w.astype(bf16)
            wg[it + 1, core, 0] = w.astype(bf16)
            gather_start(it + 1)
        else:
            new_weights[...] = w
            direction[...] = grads[ITERS]

        ag_sent(it).wait_send()
        cp_all().wait_send()
        ar_all(it).wait_send()
        for g in range(GROUPS):
            fw_copy(it, g, core).wait_send()
            sb_copy(g).wait_send()


def finish(w, d, w_out, d_out):
    w_out[...] = w[...]
    d_out[...] = d[...]


def per_device(ne, nf, features, labels, start_weights, hist_s, hist_y):
    nd = ne * nf
    chips = nd // 2
    bits = nd.bit_length() - 1
    examples = features.shape[0]
    size = start_weights.shape[0]
    pairs = hist_s.shape[0]
    rows = size // LANES
    f32, bf16 = jnp.float32, jnp.bfloat16
    vmem, dma = pltpu.VMEM, pltpu.SemaphoreType.DMA
    block = jax.ShapeDtypeStruct((rows, LANES), f32)
    in_vmem = pl.BlockSpec(memory_space=pltpu.VMEM)
    in_hbm = pl.BlockSpec(memory_space=pl.ANY)
    out = pl.pallas_call(
        functools.partial(kernel, ne, nf),
        out_shape=(block, block),
        in_specs=[in_hbm] * 5,
        out_specs=(in_vmem, in_vmem),
        scratch_shapes=[
            vmem(features.shape, bf16),
            vmem(hist_s.shape, f32),
            vmem(hist_y.shape, f32),
            vmem((1, examples), jnp.int32),
            vmem((ITERS, rows, LANES), bf16),
            vmem((2 * ITERS, rows, LANES), f32),
            vmem((ITERS, 2, chips, rows, LANES), bf16),
            vmem((ITERS, chips, rows, LANES), f32),
            vmem((ITERS, chips, rows, LANES), f32),
            vmem((chips, rows, LANES), f32),
            vmem((ITERS, chips, rows, LANES), bf16),
            vmem((ITERS, chips, rows, LANES), bf16),
            vmem((2 * ITERS, rows, LANES), f32),
            vmem((ITERS, 1, LANES), f32),
            vmem((ITERS, nd, 1, LANES), f32),
            vmem((bits + 1, pairs, LANES), f32),
            vmem((bits, pairs, LANES), f32),
            vmem((pairs, pairs, LANES), f32),
            vmem((pairs, pairs, LANES), f32),
            vmem((pairs, pairs, LANES), f32),
            dma((8,)), dma((4,)),
            dma((ITERS,)), dma((ITERS, GROUPS)),
            dma((ITERS, GROUPS)), dma((ITERS, GROUPS)),
            dma((ITERS, GROUPS)), dma((ITERS, GROUPS)),
            dma((ITERS,)), dma((ITERS,)),
            dma((ITERS,)), dma((ITERS,)),
            dma((bits,)), dma((bits,)),
        ],
        compiler_params=pltpu.CompilerParams(collective_id=0, has_side_effects=True),
    )(features, labels.reshape(1, examples), start_weights.reshape(rows, LANES), hist_s, hist_y)
    out = pl.pallas_call(finish, out_shape=(block, block), in_specs=[in_vmem] * 2,
                         out_specs=(in_vmem, in_vmem))(*out)
    return out[0].reshape(size), out[1].reshape(size)


def solution(mesh):
    return jax.shard_map(
        functools.partial(per_device, mesh.shape["ex"], mesh.shape["ft"]),
        mesh=mesh,
        in_specs=(
            P(("ex", "ft"), None),
            P(("ex", "ft")),
            P(("ex", "ft")),
            P(None, ("ex", "ft")),
            P(None, ("ex", "ft")),
        ),
        out_specs=(P(("ex", "ft")), P(("ex", "ft"))),
        check_vma=False,
    )
```
